32 devices in a mesh: gx: 8 (over y, x, core), gz: 4 (over z).
Axes of the slice: x: 2, y: 2, z: 4, core: 2. Of those that a mesh axis runs over, the one named last changes fastest.
Arguments:
- velocity: float32 [3, 64, 64, 512], P(None, 'gx', None, 'gz'), may hold values from -40 to 40
Outputs:
- coefficient: float32 [64], replicated
- eddy_viscosity: float32 [64, 64, 512], P('gx', None, 'gz')
The draws below stay inside these ranges and needn't reach their ends.
All inputs are finite; a program needn't handle non-finite values.
Results may differ from the reference program's by a relative error of at most 0.0001.
Values sent between devices are 32-bit elements; how exact they have to be, the bound alone decides.
A program may use at most 64 MiB of HBM per device.

```python
import jax
import jax.numpy as jnp
from jax import lax

NY = 64
NX = 64
NZ = 512


def draw_velocity(key, part):
    key_list = jax.random.split(key, 1)
    x_frac = jnp.arange(NX, dtype=jnp.float32) / NX
    z_frac = jnp.arange(NZ, dtype=jnp.float32) / NZ
    rising = jnp.exp(jnp.log(1.5) * (x_frac[:, None, None] + z_frac[None, None, :]))
    field = jax.random.truncated_normal(key_list[0], -6.0, 6.0, (3, NX, NY, NZ), jnp.float32) * rising
    return field.astype(jnp.float32)


def setup_inputs(seed: int = 0) -> dict:
    keys = jax.random.split(jax.random.key(seed), 2)
    velocity = draw_velocity(jax.random.fold_in(keys[1], 71), 0)
    return dict(velocity=velocity)


index_pairs = ((0, 0), (1, 1), (2, 2), (0, 1), (0, 2), (1, 2))
pair_weights = (1.0, 1.0, 1.0, 2.0, 2.0, 2.0)

def trim_edges(field):
    return field[..., 1:-1, :, 1:-1]

def along_x(field):
    return 0.5 * (field[..., 2:, :, 1:-1] - field[..., :-2, :, 1:-1])

def along_z(field):
    return 0.5 * (field[..., 1:-1, :, 2:] - field[..., 1:-1, :, :-2])

def along_y(field):
    inside = trim_edges(field)
    middle = 0.5 * (inside[..., 2:, :] - inside[..., :-2, :])
    bottom = inside[..., 1:2, :] - inside[..., 0:1, :]
    upper_end = inside[..., -1:, :] - inside[..., -2:-1, :]
    return jnp.concatenate([bottom, middle, upper_end], axis=-2)

def strain(velocity):
    gradients = [along_x(velocity), along_y(velocity), along_z(velocity)]
    strain_rate = jnp.stack([0.5 * (gradients[col_idx][row_idx] + gradients[row_idx][col_idx]) for row_idx, col_idx in index_pairs])
    weights = jnp.array(pair_weights, dtype=jnp.float32)[:, None, None, None]
    magnitude = jnp.sqrt(2.0 * lax.optimization_barrier(jnp.sum(weights * strain_rate * strain_rate, axis=0)))
    return (strain_rate, magnitude)

def box_filter(field):
    streamwise = 0.25 * (field[..., :-2, :, :] + 2.0 * field[..., 1:-1, :, :] + field[..., 2:, :, :])
    return 0.25 * (streamwise[..., :-2] + 2.0 * streamwise[..., 1:-1] + streamwise[..., 2:])

def wrap_pad(field):
    return jnp.pad(field, ((0, 0), (1, 1), (0, 0), (1, 1)), mode='wrap')

def reference(velocity):
    strain_rate, magnitude = strain(wrap_pad(velocity))
    filt_vel = box_filter(wrap_pad(velocity))
    test_rate, test_mag = strain(wrap_pad(filt_vel))
    numer = jnp.zeros((NY,), jnp.float32)
    denom = jnp.zeros((NY,), jnp.float32)
    for slot, (row_idx, col_idx) in enumerate(index_pairs):
        product = (velocity[row_idx] * velocity[col_idx])[None]
        filt_prod = box_filter(wrap_pad(product))[0]
        stress = (magnitude * strain_rate[slot])[None]
        filt_stress = box_filter(wrap_pad(stress))[0]
        leonard = filt_prod - filt_vel[row_idx] * filt_vel[col_idx]
        model_term = 2.0 * (filt_stress - 4.0 * test_mag * test_rate[slot])
        numer = numer + pair_weights[slot] * lax.optimization_barrier(jnp.sum(leonard * model_term, axis=(0, 2)))
        denom = denom + pair_weights[slot] * lax.optimization_barrier(jnp.sum(model_term * model_term, axis=(0, 2)))
    cells = NX * NZ
    coefficient = numer / cells / (denom / cells + 1e-06)
    eddy_viscosity = coefficient[None, :, None] * magnitude
    return (coefficient, eddy_viscosity)
```

```python
import functools

import jax
import jax.numpy as jnp
from jax import lax
from jax.experimental import pallas as pl
from jax.experimental.pallas import tpu as pltpu
from jax.sharding import PartitionSpec as P

pairs = ((0, 0), (1, 1), (2, 2), (0, 1), (0, 2), (1, 2))
PAD = 8
TINY = 1.1754943508222875e-38
MESH = pl.DeviceIdType.MESH


def shear_terms(dx, dy, dz, scale):
    terms = (dx[0], dy[1], dz[2], dx[1] + dy[0], dx[2] + dz[0], dy[2] + dz[1])
    square = [term * term for term in terms]
    total = (0.5 * scale) * (square[0] + square[1] + square[2]) + (0.25 * scale) * (
        square[3] + square[4] + square[5]
    )
    return terms, total * lax.rsqrt(jnp.maximum(total, TINY))


def z_parts(u, plus, minus):
    twice = [f + f for f in u]
    zs = [(plus[i] + minus[i]) + twice[i] for i in range(3)]
    dz = [plus[i] - minus[i] for i in range(3)]
    pz = [(plus[i] * plus[j] + minus[i] * minus[j]) + twice[i] * u[j] for i, j in pairs]
    return zs, dz, pz


def contraction(leonard, model):
    numer = leonard[0] * model[0]
    for slot in range(1, 6):
        numer = numer + leonard[slot] * model[slot]
    square = [term * term for term in model]
    denom = (square[0] + square[1] + square[2]) + 0.5 * (square[3] + square[4] + square[5])
    return numer, denom


def kernel(
    axes, sizes, vel, sums_out, mag_out,
    U, ZS, DZ, PZ, HU, ST, MAG, ACC,
    ZT, ZB, RT, RB, EX, GX, GL, GR, WZ, WP, WS, WH, WM, WD, BACK, GOT,
    load_sem, send_sem, recv_sem, sum_send, sum_recv, row_sem,
):
    nx, nz = sizes
    count = nx * nz
    gx, gz = lax.axis_index(axes[0]), lax.axis_index(axes[1])
    X, Y, Z = vel.shape[1:]
    W = X + 4
    half = X // 2
    xl, xr = lax.rem(gx + nx - 1, nx), lax.rem(gx + 1, nx)
    zl, zr = lax.rem(gz + nz - 1, nz), lax.rem(gz + 1, nz)
    rows = pl.ds(PAD, Y)
    me = gx * nz + gz

    load = pltpu.make_async_copy(vel, U.at[:, pl.ds(2, X), rows, :], load_sem)
    load.start()

    def to_line(body, size, peer):
        def step(k, carry):
            body(peer(k))
            return carry

        lax.fori_loop(1, size, step, 0, unroll=min(size - 1, 31))

    def in_row(k):
        return (lax.rem(gx + k, nx), gz)

    def in_column(k):
        return (gx, lax.rem(gz + k, nz))

    def anywhere(k):
        return (lax.rem(gx + k // nz, nx), lax.rem(gz + lax.rem(k, nz), nz))

    def signal(sem):
        return lambda peer: pl.semaphore_signal(sem, inc=1, device_id=peer, device_id_type=MESH)

    barrier = pltpu.get_barrier_semaphore()
    to_line(signal(barrier), nz, in_column)
    to_line(signal(barrier), nx, in_row)

    def send(slot, src, dst, peer):
        copy = pltpu.make_async_remote_copy(
            src_ref=src, dst_ref=dst, send_sem=send_sem.at[slot], recv_sem=recv_sem.at[slot],
            device_id=peer, device_id_type=MESH,
        )
        copy.start()
        return copy

    def send_plane(slot, x, ext, peer):
        src = U.at[:, pl.ds(x + 2, 1), rows, :]
        return send(slot, src, U.at[:, pl.ds(ext, 1), rows, :], peer)

    load.wait()

    tile = (8, 2 * Y)
    sub = lax.broadcasted_iota(jnp.int32, tile, 0)
    lane = lax.broadcasted_iota(jnp.int32, tile, 1)
    top, left = sub < 4, lane < Y

    def swap(f):
        return pltpu.roll(f, Y, 1)

    def turn(f):
        return pltpu.roll(f, 4, 0)

    for c in range(3):
        low, high = [], []
        for k in range(half):
            both = [U[c, 2 + k + side * half, PAD:PAD + Y, :] for side in range(2)]
            turned = jnp.concatenate(both, axis=0).T
            low.append(turned[:8])
            high.append(turned[Z - 8:])
        for j in range(half // 2):
            ZT[c, j] = jnp.where(top, turn(high[2 * j]), high[2 * j + 1])
            ZB[c, j] = jnp.where(top, low[2 * j], turn(low[2 * j + 1]))
        last = half // 2 - 1
        EX[0, c] = jnp.where(left, ZT[c, 0], swap(ZB[c, 0]))
        EX[1, c] = jnp.where(left, swap(ZT[c, last]), ZB[c, last])

    pl.semaphore_wait(barrier, nx + nz - 2)
    beside = [send(0, EX.at[0], GX.at[1], (xl, gz)), send(1, EX.at[1], GX.at[0], (xr, gz))]
    edges = [send(2, ZT, RT, (gx, zr)), send(3, ZB, RB, (gx, zl))]
    near = [send_plane(4, 0, X + 2, (xl, gz)), send_plane(5, X - 1, 1, (xr, gz))]
    far = [send_plane(6, 1, X + 3, (xl, gz)), send_plane(7, X - 2, 0, (xr, gz))]
    to_line(signal(row_sem), nx, in_row)

    def ghosts(ref, planes):
        end = PAD + Y
        for p in planes:
            for c in range(3):
                ref[c, p, PAD - 1:PAD, :] = (
                    2.0 * ref[c, p, PAD:PAD + 1, :] - ref[c, p, PAD + 1:PAD + 2, :]
                )
                ref[c, p, end:end + 1, :] = (
                    2.0 * ref[c, p, end - 1:end, :] - ref[c, p, end - 2:end - 1, :]
                )

    def ahead(f):
        return pltpu.roll(f, Z - 1, 1)

    def behind(f):
        return pltpu.roll(f, 1, 1)

    kept = {2: 0, X + 1: 1, 1: 2, X + 2: 3}

    def along_z(p, r, slope):
        q = slice(r, r + 8)
        u = [U[i, p, PAD + r:PAD + r + 8, :] for i in range(3)]
        zs, dz, pz = z_parts(u, [ahead(f) for f in u], [behind(f) for f in u])
        for i in range(3):
            ZS[i, p, q, :] = zs[i]
        if 1 <= p <= X + 2:
            for slot in range(6):
                PZ[slot, p, q, :] = pz[slot]
        if p in kept:
            for i in range(3):
                DZ[i, kept[p], q, :] = dz[i]
        slope[p] = dz

    def rates(p, r, slope):
        q = slice(r, r + 8)
        m = PAD + r
        dx = [U[i, p + 1, m:m + 8, :] - U[i, p - 1, m:m + 8, :] for i in range(3)]
        dy = [U[i, p, m + 1:m + 9, :] - U[i, p, m - 1:m + 7, :] for i in range(3)]
        dz = slope[p] if p in slope else [DZ[i, kept[p], q, :] for i in range(3)]
        terms, mag = shear_terms(dx, dy, dz, 1.0)
        MAG[p, q, :] = mag
        for slot in range(6):
            ST[slot, p, q, :] = mag * terms[slot]

    def smooth(planes, r):
        q = slice(r, r + 8)
        for i in range(3):
            pair = {}
            for p in planes:
                for s in (p - 1, p):
                    if s not in pair:
                        pair[s] = ZS[i, s, q, :] + ZS[i, s + 1, q, :]
                HU[i, p, PAD + r:PAD + r + 8, :] = 0.25 * (pair[p - 1] + pair[p])

    def stage_a(z_planes, planes):
        for r in range(0, Y, 8):
            slope = {}
            for p in z_planes:
                along_z(p, r, slope)
            for p in planes:
                rates(p, r, slope)
            smooth(planes, r)
        ghosts(HU, planes)

    def test_side(h, dx, dy, dz, px, sz):
        terms, mag = shear_terms(dx, dy, dz, 16.0)
        leonard = [px[slot] - h[i] * h[j] for slot, (i, j) in enumerate(pairs)]
        model = [sz[slot] - mag * terms[slot] for slot in range(6)]
        return contraction(leonard, model)

    def stage_b(planes):
        for r in range(0, Y, 8):
            q = slice(r, r + 8)
            m = PAD + r
            pair = {}

            def x_sum(ref, slot, p):
                for s in (p - 1, p):
                    if (id(ref), slot, s) not in pair:
                        pair[id(ref), slot, s] = ref[slot, s, q, :] + ref[slot, s + 1, q, :]
                return pair[id(ref), slot, p - 1] + pair[id(ref), slot, p]

            total = None
            for p in planes:
                h = [HU[i, p, m:m + 8, :] for i in range(3)]
                dx = [HU[i, p + 1, m:m + 8, :] - HU[i, p - 1, m:m + 8, :] for i in range(3)]
                dy = [HU[i, p, m + 1:m + 9, :] - HU[i, p, m - 1:m + 7, :] for i in range(3)]
                dz = [ahead(f) - behind(f) for f in h]
                px = [x_sum(PZ, slot, p) for slot in range(6)]
                sz = []
                for slot in range(6):
                    sx = x_sum(ST, slot, p)
                    two = sx + behind(sx)
                    sz.append(two + ahead(two))
                found = test_side(h, dx, dy, dz, px, sz)
                total = found if total is None else [a + b for a, b in zip(total, found)]
            ACC[q, :] += total[0]
            ACC[r + Y:r + Y + 8, :] += total[1]

    ACC[...] = jnp.zeros_like(ACC)
    WD[...] = jnp.zeros_like(WD)
    own = range(2, X + 2)
    ghosts(U, own)
    stage_a(own, range(3, X + 1))
    stage_b(range(4, X))

    for copy in beside:
        copy.wait_recv()
    corners = [send(8, GX, GL, (gx, zr)), send(9, GX, GR, (gx, zl))]

    for copy in near:
        copy.wait_recv()
    ghosts(U, (1, X + 2))
    stage_a((1, X + 2), (2, X + 1))
    stage_b((3,))
    stage_b((X,))

    y = lane - jnp.where(left, 0, Y)
    plus_by = jnp.where(y == 0, 2.0, jnp.where(y == Y - 1, 0.0, 1.0))
    minus_by = jnp.where(y == 0, 0.0, jnp.where(y == Y - 1, 2.0, 1.0))
    self_by = jnp.where(y == 0, -2.0, jnp.where(y == Y - 1, 2.0, 0.0))

    def y_diff(f):
        plus, minus = pltpu.roll(f, 2 * Y - 1, 1), pltpu.roll(f, 1, 1)
        return (plus_by * plus - minus_by * minus) + self_by * f

    def up(f):
        return pltpu.roll(f, 7, 0)

    def down(f):
        return pltpu.roll(f, 1, 0)

    def join(odd, first, second):
        return jnp.where(top, turn(first) if odd else first, second if odd else turn(second))

    def window_a(cells, planes):
        slope = {}
        for p in cells:
            u = cells[p]
            zs, dz, pz = z_parts(u, [up(f) for f in u], [down(f) for f in u])
            for i in range(3):
                WZ[i, p] = zs[i]
                WZ[3 + i, p] = u[i]
                WZ[6 + i, p] = dz[i]
            for slot in range(6):
                WP[slot, p] = pz[slot]
        for p in planes:
            dx = [WZ[3 + i, p + 1] - WZ[3 + i, p - 1] for i in range(3)]
            dy = [y_diff(WZ[3 + i, p]) for i in range(3)]
            dz = [WZ[6 + i, p] for i in range(3)]
            terms, mag = shear_terms(dx, dy, dz, 1.0)
            WM[p] = mag
            for slot in range(6):
                WS[slot, p] = mag * terms[slot]
            for i in range(3):
                WH[i, p] = 0.25 * ((WZ[i, p - 1] + WZ[i, p]) + (WZ[i, p] + WZ[i, p + 1]))

    def window_b(planes):
        total = None
        for p in planes:
            h = [WH[i, p] for i in range(3)]
            dx = [WH[i, p + 1] - WH[i, p - 1] for i in range(3)]
            dy = [y_diff(f) for f in h]
            dz = [up(f) - down(f) for f in h]
            px = [(WP[s, p - 1] + WP[s, p]) + (WP[s, p] + WP[s, p + 1]) for s in range(6)]
            sz = []
            for s in range(6):
                two = (WS[s, p - 1] + WS[s, p]) + (WS[s, p] + WS[s, p + 1])
                two = two + down(two)
                sz.append(two + up(two))
            found = test_side(h, dx, dy, dz, px, sz)
            total = found if total is None else [a + b for a, b in zip(total, found)]
        WD[0] += total[0]
        WD[1] += total[1]

    for copy in edges:
        copy.wait_recv()
    cells = {p: [] for p in own}
    for c in range(3):
        for j in range(half // 2):
            rt, zt, zb, rb = RT[c, j], ZT[c, j], ZB[c, j], RB[c, j]
            first = (jnp.where(left, rt, swap(zt)), jnp.where(left, swap(rt), zt))
            second = (jnp.where(left, zb, swap(rb)), jnp.where(left, swap(zb), rb))
            for odd in range(2):
                for side in range(2):
                    cells[2 + 2 * j + odd + side * half].append(join(odd, first[side], second[side]))
    window_a(cells, range(3, X + 1))
    window_b(range(4, X))

    for copy in far:
        copy.wait_recv()
    ghosts(U, (0, X + 3))
    stage_a((0, X + 3), (1, X + 2))
    stage_b((2,))
    stage_b((X + 1,))

    for copy in corners:
        copy.wait_recv()
    cells = {0: [], 1: [], X + 2: [], X + 3: []}
    for c in range(3):
        for side in range(2):
            mine, lower, upper = swap(GX[side, c]), GL[side, c], GR[side, c]
            first, second = jnp.where(left, lower, mine), jnp.where(left, mine, upper)
            for odd in range(2):
                cells[side * (X + 2) + odd].append(join(odd, first, second))
    window_a(cells, (1, 2, X + 1, X + 2))
    window_b((2, 3, X, X + 1))

    take = (left & ((sub == 4) | (sub == 5))) | (~left & ((sub == 2) | (sub == 3)))
    numer = jnp.sum(jnp.where(take, WD[0], 0.0), axis=0, keepdims=True)
    denom = jnp.sum(jnp.where(take, WD[1], 0.0), axis=0, keepdims=True)
    numer = numer + swap(numer)
    denom = denom + swap(denom)
    window_sums = jnp.where(left[:1], numer, denom)
    turned = jnp.sum(ACC[...].T[2:Z - 2], axis=0, keepdims=True)
    GOT[me] = window_sums + turned

    def total_copy(peer):
        return pltpu.make_async_remote_copy(
            src_ref=GOT.at[me], dst_ref=GOT.at[me], send_sem=sum_send, recv_sem=sum_recv,
            device_id=peer, device_id_type=MESH,
        )

    pl.semaphore_wait(row_sem, nx - 1)
    to_line(lambda peer: total_copy(peer).start(), count, anywhere)

    back = jnp.concatenate([WM[p] for p in own], axis=0)
    back = jnp.concatenate([back, jnp.zeros((Z - 8 * X, 2 * Y), jnp.float32)], axis=0).T
    BACK[...] = back
    spot = lax.broadcasted_iota(jnp.int32, (Y, Z), 1)
    for x in range(X):
        low_lane = pltpu.roll(BACK[:Y], (Z - 8 * x - 4) % Z, 1)
        high_lane = pltpu.roll(BACK[Y:], (Z - 1 - 8 * x - 3) % Z, 1)
        mag = MAG[x + 2]
        mag_out[x] = jnp.where(spot == 0, low_lane, jnp.where(spot == Z - 1, high_lane, mag))
    for copy in beside + edges + near + far + corners:
        copy.wait_send()
    everyone = GOT.at[pl.ds(0, count - 1)]
    pltpu.make_async_copy(everyone, everyone, sum_recv).wait()
    sums_out[...] = jnp.sum(GOT[...], axis=0)
    pltpu.make_async_copy(everyone, everyone, sum_send).wait()


def finish(cells, sums, mag, coef_out, visc_out):
    X, Y, Z = mag.shape
    total = sums[...] * (1.0 / (256.0 * cells))
    coef = total / (pltpu.roll(total, Y, 1) + 1e-6)
    coef_out[...] = coef[0, :Y]
    wide = jnp.broadcast_to(coef, (Z, 2 * Y)).T[:Y]
    for x in range(X):
        visc_out[x] = wide * mag[x]


def on_device(axes, sizes, velocity):
    X, Y, Z = velocity.shape[1:]
    nx, nz = sizes
    f32 = jnp.float32
    tall = Y + 2 * PAD
    W = X + 4
    dma = pltpu.SemaphoreType.DMA
    cells = X * nx * Z * nz
    vmem = pl.BlockSpec(memory_space=pltpu.VMEM)
    strip = pltpu.VMEM((3, X // 4, 8, 2 * Y), f32)
    ends = pltpu.VMEM((2, 3, 8, 2 * Y), f32)
    sums, mag = pl.pallas_call(
        functools.partial(kernel, axes, sizes),
        out_shape=(pltpu.VMEM((1, 2 * Y), f32), pltpu.VMEM((X, Y, Z), f32)),
        in_specs=[pl.BlockSpec(memory_space=pl.ANY)],
        out_specs=(vmem, vmem),
        scratch_shapes=[
            pltpu.VMEM((3, W, tall, Z), f32),
            pltpu.VMEM((3, W, Y, Z), f32),
            pltpu.VMEM((3, 4, Y, Z), f32),
            pltpu.VMEM((6, W, Y, Z), f32),
            pltpu.VMEM((3, W, tall, Z), f32),
            pltpu.VMEM((6, W, Y, Z), f32),
            pltpu.VMEM((W, Y, Z), f32),
            pltpu.VMEM((2 * Y, Z), f32),
            strip,
            strip,
            strip,
            strip,
            ends,
            ends,
            ends,
            ends,
            pltpu.VMEM((9, W, 8, 2 * Y), f32),
            pltpu.VMEM((6, W, 8, 2 * Y), f32),
            pltpu.VMEM((6, W, 8, 2 * Y), f32),
            pltpu.VMEM((3, W, 8, 2 * Y), f32),
            pltpu.VMEM((W, 8, 2 * Y), f32),
            pltpu.VMEM((2, 8, 2 * Y), f32),
            pltpu.VMEM((2 * Y, Z), f32),
            pltpu.VMEM((nx * nz, 1, 2 * Y), f32),
            dma,
            dma((10,)),
            dma((10,)),
            dma,
            dma,
            pltpu.SemaphoreType.REGULAR,
        ],
        compiler_params=pltpu.CompilerParams(collective_id=0, has_side_effects=True),
    )(velocity)
    return pl.pallas_call(
        functools.partial(finish, cells),
        out_shape=(jax.ShapeDtypeStruct((Y,), f32), jax.ShapeDtypeStruct((X, Y, Z), f32)),
        in_specs=[vmem, vmem],
        out_specs=(vmem, vmem),
    )(*(pltpu.with_memory_space_constraint(a, pltpu.VMEM) for a in (sums, mag)))


def solution(mesh):
    axes = ("gx", "gz")
    sizes = tuple(mesh.shape[axis] for axis in axes)
    return jax.shard_map(
        functools.partial(on_device, axes, sizes),
        mesh=mesh,
        in_specs=(P(None, "gx", None, "gz"),),
        out_specs=(P(), P("gx", None, "gz")),
        check_vma=False,
    )
```

```python
import functools

import jax
import jax.numpy as jnp
from jax import lax
from jax.experimental import pallas as pl
from jax.experimental.pallas import tpu as pltpu
from jax.sharding import PartitionSpec as P

pairs = ((0, 0), (1, 1), (2, 2), (0, 1), (0, 2), (1, 2))
PAD = 8
TINY = 1.1754943508222875e-38
MESH = pl.DeviceIdType.MESH


def shear_terms(dx, dy, dz, scale):
    terms = (dx[0], dy[1], dz[2], dx[1] + dy[0], dx[2] + dz[0], dy[2] + dz[1])
    square = [term * term for term in terms]
    total = (0.5 * scale) * (square[0] + square[1] + square[2]) + (0.25 * scale) * (
        square[3] + square[4] + square[5]
    )
    return terms, total * lax.rsqrt(jnp.maximum(total, TINY))


def z_parts(u, plus, minus):
    twice = [f + f for f in u]
    zs = [(plus[i] + minus[i]) + twice[i] for i in range(3)]
    dz = [plus[i] - minus[i] for i in range(3)]
    pz = [(plus[i] * plus[j] + minus[i] * minus[j]) + twice[i] * u[j] for i, j in pairs]
    return zs, dz, pz


def contraction(leonard, model):
    numer = leonard[0] * model[0]
    for slot in range(1, 6):
        numer = numer + leonard[slot] * model[slot]
    square = [term * term for term in model]
    denom = (square[0] + square[1] + square[2]) + 0.5 * (square[3] + square[4] + square[5])
    return numer, denom


def knowledge_rounds(size):
    reach, columns, rounds = 1, 0, []
    while reach < size // 2 or columns < size // 2:
        step = min(reach, 2 * columns + 1, size // 2 - columns)
        rounds.append(step)
        reach, columns = reach + step, columns + step
    return rounds


def kernel(
    axes, sizes, vel, sums_out, mag_out,
    U, ZS, DZ, PZ, HU, ST, MAG, ACC,
    ZT, ZB, RT, RB, EX, GX, GL, GR, WZ, WP, WS, WH, WM, WD, BACK, GOT,
    load_sem, send_sem, recv_sem, sum_send, sum_recv, row_sem, wrap_sem, all_sem,
):
    nx, nz = sizes
    count = nx * nz
    gx, gz = lax.axis_index(axes[0]), lax.axis_index(axes[1])
    X, Y, Z = vel.shape[1:]
    W = X + 4
    half = X // 2
    xl, xr = lax.rem(gx + nx - 1, nx), lax.rem(gx + 1, nx)
    zl, zr = lax.rem(gz + nz - 1, nz), lax.rem(gz + 1, nz)
    rows = pl.ds(PAD, Y)
    me = gx * nz + gz

    loads = [
        pltpu.make_async_copy(
            vel.at[:, pl.ds(x, size)], U.at[:, pl.ds(x + 2, size), rows, :], load_sem.at[slot]
        )
        for slot, (x, size) in enumerate(((0, 2), (X - 2, 2), (2, X - 4)))
    ]
    for load in loads:
        load.start()

    def to_line(body, size, peer):
        def step(k, carry):
            body(peer(k))
            return carry

        lax.fori_loop(1, size, step, 0, unroll=min(size - 1, 31))

    def anywhere(k):
        spot = gz * nx + gx
        peer = k - 1 + jnp.where(k > spot, 1, 0)
        return (lax.rem(peer, nx), peer // nx)

    def signal(sem):
        return lambda peer: pl.semaphore_signal(sem, inc=1, device_id=peer, device_id_type=MESH)

    barrier = pltpu.get_barrier_semaphore()
    for peer in ((xl, gz), (xr, gz)):
        signal(barrier)(peer)

    def to_column(sem, distance):
        @pl.when((gz + distance >= 0) & (gz + distance < nz))
        def _():
            signal(sem)((gx, gz + distance))

    to_column(barrier, -1)
    for distance in range(1, nz):
        to_column(barrier, distance)

    def send(slot, src, dst, peer):
        copy = pltpu.make_async_remote_copy(
            src_ref=src, dst_ref=dst, send_sem=send_sem.at[slot], recv_sem=recv_sem.at[slot],
            device_id=peer, device_id_type=MESH,
        )
        return copy

    deep = Y // 2
    parts = ((0, Y, 1), (0, deep, 0), (deep, deep, 0))

    def halo_copy(part, side, ext, dst, peer):
        first, size, _ = parts[part]
        span = pl.ds(PAD + first, size)
        slot = 4 + 2 * part + side
        return pltpu.make_async_remote_copy(
            src_ref=U.at[:, pl.ds(ext, 1), span, :], dst_ref=U.at[:, pl.ds(dst, 1), span, :],
            send_sem=send_sem.at[slot], recv_sem=recv_sem.at[slot], device_id=peer, device_id_type=MESH,
        )

    tile = (8, 2 * Y)
    sub = lax.broadcasted_iota(jnp.int32, tile, 0)
    lane = lax.broadcasted_iota(jnp.int32, tile, 1)
    top, left = sub < 4, lane < Y

    def swap(f):
        return pltpu.roll(f, Y, 1)

    def turn(f):
        return pltpu.roll(f, 4, 0)

    def partner(k):
        return X - 2 + k if k < 2 else half + k - 2

    def strips(j):
        for c in range(3):
            low, high = [], []
            for k in (2 * j, 2 * j + 1):
                both = [U[c, 2 + x, PAD:PAD + Y, :] for x in (k, partner(k))]
                turned = jnp.concatenate(both, axis=0).T
                low.append(turned[:8])
                high.append(turned[Z - 8:])
            tops = jnp.where(top, turn(high[0]), high[1])
            bottoms = jnp.where(top, low[0], turn(low[1]))
            ZT[c, j] = tops
            ZB[c, j] = bottoms
            if j == 0:
                EX[0, c] = jnp.where(left, tops, swap(bottoms))
                EX[1, c] = jnp.where(left, swap(tops), bottoms)

    rounds = knowledge_rounds(nx)

    def tell(turn):
        for peer in sorted({rounds[turn] % nx, -rounds[turn] % nx}):
            signal(row_sem.at[turn])((lax.rem(gx + peer, nx), gz))

    def spread(turns):
        @pl.when(gz == nz - 1)
        def _():
            for k in turns:
                pl.semaphore_wait(row_sem.at[k], len({rounds[k] % nx, -rounds[k] % nx}))
                if k + 1 < len(rounds):
                    tell(k + 1)
                else:
                    for z in range(nz - 1):
                        signal(all_sem)((gx, z))

    pl.semaphore_wait(barrier, 2 + gz + jnp.where(gz < nz - 1, 1, 0))

    @pl.when(gz == nz - 1)
    def _():
        signal(wrap_sem)((gx, 0))
        tell(0)

    loads[0].wait()
    loads[1].wait()
    strips(0)
    beside = [send(0, EX.at[1], GX.at[0], (xr, gz)), send(1, EX.at[0], GX.at[1], (xl, gz))]
    for copy in beside:
        copy.start()
    edges = [send(2, ZT, RT, (gx, zr)), send(3, ZB, RB, (gx, zl))]
    halo = []
    for part, (_, _, ext) in enumerate(parts):
        halo.append(halo_copy(part, 0, X + ext, ext, (xr, gz)))
        halo.append(halo_copy(part, 1, 3 - ext, X + 3 - ext, (xl, gz)))
    for copy in halo:
        copy.start()
    loads[2].wait()
    for j in range(1, half // 2):
        strips(j)
    edges[0].start()

    @pl.when(gz > 0)
    def _():
        edges[1].start()

    def ghosts(ref, planes):
        end = PAD + Y
        for p in planes:
            for c in range(3):
                ref[c, p, PAD - 1:PAD, :] = (
                    2.0 * ref[c, p, PAD:PAD + 1, :] - ref[c, p, PAD + 1:PAD + 2, :]
                )
                ref[c, p, end:end + 1, :] = (
                    2.0 * ref[c, p, end - 1:end, :] - ref[c, p, end - 2:end - 1, :]
                )

    def ahead(f):
        return pltpu.roll(f, Z - 1, 1)

    def behind(f):
        return pltpu.roll(f, 1, 1)

    def along_z(p, r, slope, keep, partial):
        q = slice(r, r + 8)
        u = [U[i, p, PAD + r:PAD + r + 8, :] for i in range(3)]
        zs, dz, pz = z_parts(u, [ahead(f) for f in u], [behind(f) for f in u])
        for i in range(3):
            ZS[i, p, q, :] = zs[i]
        if not partial:
            for slot in range(6):
                PZ[slot, p, q, :] = pz[slot]
        if keep is not None:
            for i in range(3):
                DZ[i, keep, q, :] = dz[i]
        slope.append(dz)

    def rates(p, r, dz):
        q = slice(r, r + 8)
        m = PAD + r
        dx = [U[i, p + 1, m:m + 8, :] - U[i, p - 1, m:m + 8, :] for i in range(3)]
        dy = [U[i, p, m + 1:m + 9, :] - U[i, p, m - 1:m + 7, :] for i in range(3)]
        if not isinstance(dz, list):
            dz = [DZ[i, dz, q, :] for i in range(3)]
        terms, mag = shear_terms(dx, dy, dz, 1.0)
        MAG[p, q, :] = mag
        for slot in range(6):
            ST[slot, p, q, :] = mag * terms[slot]

    def smooth(planes, r):
        q = slice(r, r + 8)
        for i in range(3):
            for p in planes:
                HU[i, p, PAD + r:PAD + r + 8, :] = 0.25 * (
                    (ZS[i, p - 1, q, :] + ZS[i, p + 1, q, :]) + 2.0 * ZS[i, p, q, :]
                )

    def smooth_own(planes, r):
        q = slice(r, r + 8)
        for i in range(3):
            pair = {}
            for p in planes:
                for s in (p - 1, p):
                    if s not in pair:
                        pair[s] = ZS[i, s, q, :] + ZS[i, s + 1, q, :]
                HU[i, p, PAD + r:PAD + r + 8, :] = 0.25 * (pair[p - 1] + pair[p])

    def test_side(h, dx, dy, dz, px, sz):
        terms, mag = shear_terms(dx, dy, dz, 16.0)
        leonard = [px[slot] - h[i] * h[j] for slot, (i, j) in enumerate(pairs)]
        model = [sz[slot] - mag * terms[slot] for slot in range(6)]
        return contraction(leonard, model)

    def stage_b(spots, at, first=0, last=Y):
        for r in range(first, last, 8):
            q = slice(r, r + 8)
            m = PAD + r
            pair = {}

            def x_sum(ref, slot, k):
                for s in (k - 1, k):
                    if (id(ref), slot, s) not in pair:
                        pair[id(ref), slot, s] = ref[slot, at(s), q, :] + ref[slot, at(s + 1), q, :]
                return pair[id(ref), slot, k - 1] + pair[id(ref), slot, k]

            total = None
            for k in spots:
                p = at(k)
                h = [HU[i, p, m:m + 8, :] for i in range(3)]
                dx = [HU[i, p + 1, m:m + 8, :] - HU[i, p - 1, m:m + 8, :] for i in range(3)]
                dy = [HU[i, p, m + 1:m + 9, :] - HU[i, p, m - 1:m + 7, :] for i in range(3)]
                dz = [ahead(f) - behind(f) for f in h]
                px = [x_sum(PZ, slot, k) for slot in range(6)]
                sz = []
                for slot in range(6):
                    sx = x_sum(ST, slot, k)
                    two = sx + behind(sx)
                    sz.append(two + ahead(two))
                found = test_side(h, dx, dy, dz, px, sz)
                total = found if total is None else [a + b for a, b in zip(total, found)]
            ACC[q, :] += total[0]
            ACC[r + Y:r + Y + 8, :] += total[1]

    ACC[...] = jnp.zeros_like(ACC)
    WD[...] = jnp.zeros_like(WD)
    own = range(2, X + 2)
    ghosts(U, own)
    for r in range(0, Y, 8):
        slope = []
        for p in own:
            along_z(p, r, slope, {2: 0, X + 1: 1}.get(p), False)
        for p in own[1:-1]:
            rates(p, r, slope[p - 2])
        smooth_own(own[1:-1], r)
    ghosts(HU, own[1:-1])
    stage_b(own[2:-2], lambda k: k)

    fast = 1 - lax.rem(gx, 2)

    def arrive(side, part):
        ext = side * (X + 3) + (1 - 2 * side) * parts[part][2]
        halo_copy(part, side, ext, ext, (xl, gz)).wait_recv()

    def boundary(side, near, far, first=0, last=Y):
        def at(k):
            return side * (X + 3) + (1 - 2 * side) * k

        if near:
            ghosts(U, [at(1)])
        fresh = [at(2)] * near + [at(1)] * far
        for r in range(first, last, 8):
            slope = []
            if near:
                along_z(at(1), r, slope, None if far else 2 + side, False)
            if far:
                along_z(at(0), r, [], None, True)
            if near:
                rates(at(2), r, side)
            if far:
                rates(at(1), r, slope[0] if near else 2 + side)
            smooth(fresh, r)
        if near:
            ghosts(HU, [at(2)])
        stage_b([3] * near + [2] * far, at, first, last)

    def strip_arrives(side):
        send(side, EX.at[0], GX.at[side], (xl, gz)).wait_recv()

    def forward(side):
        return (
            send(10 + side, GX.at[side], GL.at[side], (gx, zr)),
            send(12 + side, GX.at[side], GR.at[side], (gx, zl)),
        )

    slow = 1 - fast
    spread(range(0, 1))
    strip_arrives(fast)
    corners = [*forward(fast), *forward(slow)]
    corners[0].start()

    @pl.when(gz > 0)
    def _():
        corners[1].start()

    for part in range(3):
        arrive(fast, part)
    boundary(fast, True, True)
    strip_arrives(slow)
    corners[2].start()

    @pl.when(gz == 0)
    def _():
        pl.semaphore_wait(wrap_sem, 1)
        edges[1].start()
        corners[1].start()

    corners[3].start()
    spread(range(1, 2))

    y = lane - jnp.where(left, 0, Y)
    plus_by = jnp.where(y == 0, 2.0, jnp.where(y == Y - 1, 0.0, 1.0))
    minus_by = jnp.where(y == 0, 0.0, jnp.where(y == Y - 1, 2.0, 1.0))
    self_by = jnp.where(y == 0, -2.0, jnp.where(y == Y - 1, 2.0, 0.0))

    def y_diff(f):
        plus, minus = pltpu.roll(f, 2 * Y - 1, 1), pltpu.roll(f, 1, 1)
        return (plus_by * plus - minus_by * minus) + self_by * f

    def up(f):
        return pltpu.roll(f, 7, 0)

    def down(f):
        return pltpu.roll(f, 1, 0)

    def join(odd, first, second):
        return jnp.where(top, turn(first) if odd else first, second if odd else turn(second))

    def window_a(cells, planes):
        slope = {}
        for p in cells:
            u = cells[p]
            zs, dz, pz = z_parts(u, [up(f) for f in u], [down(f) for f in u])
            for i in range(3):
                WZ[i, p] = zs[i]
                WZ[3 + i, p] = u[i]
                WZ[6 + i, p] = dz[i]
            for slot in range(6):
                WP[slot, p] = pz[slot]
        for p in planes:
            dx = [WZ[3 + i, p + 1] - WZ[3 + i, p - 1] for i in range(3)]
            dy = [y_diff(WZ[3 + i, p]) for i in range(3)]
            dz = [WZ[6 + i, p] for i in range(3)]
            terms, mag = shear_terms(dx, dy, dz, 1.0)
            WM[p] = mag
            for slot in range(6):
                WS[slot, p] = mag * terms[slot]
            for i in range(3):
                WH[i, p] = 0.25 * ((WZ[i, p - 1] + WZ[i, p]) + (WZ[i, p] + WZ[i, p + 1]))

    def window_b(planes):
        total = None
        for p in planes:
            h = [WH[i, p] for i in range(3)]
            dx = [WH[i, p + 1] - WH[i, p - 1] for i in range(3)]
            dy = [y_diff(f) for f in h]
            dz = [up(f) - down(f) for f in h]
            px = [(WP[s, p - 1] + WP[s, p]) + (WP[s, p] + WP[s, p + 1]) for s in range(6)]
            sz = []
            for s in range(6):
                two = (WS[s, p - 1] + WS[s, p]) + (WS[s, p] + WS[s, p + 1])
                two = two + down(two)
                sz.append(two + up(two))
            found = test_side(h, dx, dy, dz, px, sz)
            total = found if total is None else [a + b for a, b in zip(total, found)]
        WD[0] += total[0]
        WD[1] += total[1]

    arrive(slow, 0)
    boundary(slow, True, False)
    spread(range(2, len(rounds)))

    for copy in edges:
        copy.wait_recv()
    cells = {p: [] for p in own}
    for c in range(3):
        for j in range(half // 2):
            rt, zt, zb, rb = RT[c, j], ZT[c, j], ZB[c, j], RB[c, j]
            first = (jnp.where(left, rt, swap(zt)), jnp.where(left, swap(rt), zt))
            second = (jnp.where(left, zb, swap(rb)), jnp.where(left, swap(zb), rb))
            for odd in range(2):
                for side in range(2):
                    x = partner(2 * j + odd) if side else 2 * j + odd
                    cells[2 + x].append(join(odd, first[side], second[side]))
    window_a(cells, range(3, X + 1))
    window_b(range(4, X))

    for copy in corners:
        copy.wait_recv()
    cells = {0: [], 1: [], X + 2: [], X + 3: []}
    for c in range(3):
        for side in range(2):
            mine, lower, upper = swap(GX[side, c]), GL[side, c], GR[side, c]
            first, second = jnp.where(left, lower, mine), jnp.where(left, mine, upper)
            for odd in range(2):
                cells[side * (X + 2) + odd].append(join(odd, first, second))
    window_a(cells, (1, 2, X + 1, X + 2))
    window_b((2, 3, X, X + 1))

    arrive(slow, 1)
    boundary(slow, False, True, 0, deep)
    arrive(slow, 2)
    boundary(slow, False, True, deep, Y)

    take = (left & ((sub == 4) | (sub == 5))) | (~left & ((sub == 2) | (sub == 3)))
    numer = jnp.sum(jnp.where(take, WD[0], 0.0), axis=0, keepdims=True)
    denom = jnp.sum(jnp.where(take, WD[1], 0.0), axis=0, keepdims=True)
    numer = numer + swap(numer)
    denom = denom + swap(denom)
    window_sums = jnp.where(left[:1], numer, denom)
    turned = jnp.sum(ACC[...].T[2:Z - 2], axis=0, keepdims=True)
    GOT[me] = window_sums + turned

    def total_copy(peer):
        return pltpu.make_async_remote_copy(
            src_ref=GOT.at[me], dst_ref=GOT.at[me], send_sem=sum_send, recv_sem=sum_recv,
            device_id=peer, device_id_type=MESH,
        )


    @pl.when(gz < nz - 1)
    def _():
        pl.semaphore_wait(all_sem, 1)

    to_line(lambda peer: total_copy(peer).start(), count, anywhere)

    back = jnp.concatenate([WM[p] for p in own], axis=0)
    back = jnp.concatenate([back, jnp.zeros((Z - 8 * X, 2 * Y), jnp.float32)], axis=0).T
    BACK[...] = back
    spot = lax.broadcasted_iota(jnp.int32, (Y, Z), 1)
    for x in range(X):
        low_lane = pltpu.roll(BACK[:Y], (Z - 8 * x - 4) % Z, 1)
        high_lane = pltpu.roll(BACK[Y:], (Z - 1 - 8 * x - 3) % Z, 1)
        mag = MAG[x + 2]
        mag_out[x] = jnp.where(spot == 0, low_lane, jnp.where(spot == Z - 1, high_lane, mag))
    for copy in beside + edges + halo + corners:
        copy.wait_send()
    everyone = GOT.at[pl.ds(0, count - 1)]
    pltpu.make_async_copy(everyone, everyone, sum_recv).wait()
    sums_out[...] = jnp.sum(GOT[...], axis=0)
    pltpu.make_async_copy(everyone, everyone, sum_send).wait()


def finish(cells, sums, mag, coef_out, visc_out):
    X, Y, Z = mag.shape
    total = sums[...] * (1.0 / (256.0 * cells))
    coef = total / (pltpu.roll(total, Y, 1) + 1e-6)
    coef_out[...] = coef[0, :Y]
    wide = jnp.broadcast_to(coef, (Z, 2 * Y)).T[:Y]
    for x in range(X):
        visc_out[x] = wide * mag[x]


def on_device(axes, sizes, velocity):
    X, Y, Z = velocity.shape[1:]
    nx, nz = sizes
    f32 = jnp.float32
    tall = Y + 2 * PAD
    W = X + 4
    dma = pltpu.SemaphoreType.DMA
    cells = X * nx * Z * nz
    vmem = pl.BlockSpec(memory_space=pltpu.VMEM)
    strip = pltpu.VMEM((3, X // 4, 8, 2 * Y), f32)
    ends = pltpu.VMEM((2, 3, 8, 2 * Y), f32)
    sums, mag = pl.pallas_call(
        functools.partial(kernel, axes, sizes),
        out_shape=(pltpu.VMEM((1, 2 * Y), f32), pltpu.VMEM((X, Y, Z), f32)),
        in_specs=[pl.BlockSpec(memory_space=pl.ANY)],
        out_specs=(vmem, vmem),
        scratch_shapes=[
            pltpu.VMEM((3, W, tall, Z), f32),
            pltpu.VMEM((3, W, Y, Z), f32),
            pltpu.VMEM((3, 4, Y, Z), f32),
            pltpu.VMEM((6, W, Y, Z), f32),
            pltpu.VMEM((3, W, tall, Z), f32),
            pltpu.VMEM((6, W, Y, Z), f32),
            pltpu.VMEM((W, Y, Z), f32),
            pltpu.VMEM((2 * Y, Z), f32),
            strip,
            strip,
            strip,
            strip,
            ends,
            ends,
            ends,
            ends,
            pltpu.VMEM((9, W, 8, 2 * Y), f32),
            pltpu.VMEM((6, W, 8, 2 * Y), f32),
            pltpu.VMEM((6, W, 8, 2 * Y), f32),
            pltpu.VMEM((3, W, 8, 2 * Y), f32),
            pltpu.VMEM((W, 8, 2 * Y), f32),
            pltpu.VMEM((2, 8, 2 * Y), f32),
            pltpu.VMEM((2 * Y, Z), f32),
            pltpu.VMEM((nx * nz, 1, 2 * Y), f32),
            dma((3,)),
            dma((14,)),
            dma((14,)),
            dma,
            dma,
            pltpu.SemaphoreType.REGULAR((len(knowledge_rounds(nx)),)),
            pltpu.SemaphoreType.REGULAR,
            pltpu.SemaphoreType.REGULAR,
        ],
        compiler_params=pltpu.CompilerParams(collective_id=0, has_side_effects=True),
    )(velocity)
    return pl.pallas_call(
        functools.partial(finish, cells),
        out_shape=(jax.ShapeDtypeStruct((Y,), f32), jax.ShapeDtypeStruct((X, Y, Z), f32)),
        in_specs=[vmem, vmem],
        out_specs=(vmem, vmem),
    )(*(pltpu.with_memory_space_constraint(a, pltpu.VMEM) for a in (sums, mag)))


def solution(mesh):
    axes = ("gx", "gz")
    sizes = tuple(mesh.shape[axis] for axis in axes)
    return jax.shard_map(
        functools.partial(on_device, axes, sizes),
        mesh=mesh,
        in_specs=(P(None, "gx", None, "gz"),),
        out_specs=(P(), P("gx", None, "gz")),
        check_vma=False,
    )
```
